32 devices in a mesh: cand: 4 (over y, core), tensor: 8 (over z, x).
Axes of the slice: x: 2, y: 2, z: 4, core: 2. Of those that a mesh axis runs over, the one named last changes fastest.
Arguments:
- states: bfloat16 [512, 3584], P('cand'), may hold values from -60 to 60
- targets: int32 [512], replicated, may hold values from 0 to 131071
- loss_mask: int32 [512], P('cand'), may hold values 0 or 1
- cand_of: int32 [4], replicated, may hold values from 0 to 3
- lambdas: float32 [4], replicated, may hold values from 0.2 to 1
- base_q: bfloat16 [3584, 4096], P('cand', 'tensor'), may hold values from -0.09375 to 0.09375
- delta_q: bfloat16 [2, 3584, 4096], P(None, 'cand', 'tensor'), may hold values from -0.046875 to 0.046875
- base_k: bfloat16 [3584, 2048], P('cand'), may hold values from -0.09375 to 0.09375
- delta_k: bfloat16 [2, 3584, 2048], P(None, 'cand'), may hold values from -0.046875 to 0.046875
- base_v: bfloat16 [3584, 2048], P('cand'), may hold values from -0.09375 to 0.09375
- delta_v: bfloat16 [2, 3584, 2048], P(None, 'cand'), may hold values from -0.046875 to 0.046875
- base_o: bfloat16 [4096, 3584], P('tensor', 'cand'), may hold values from -0.09375 to 0.09375
- delta_o: bfloat16 [2, 4096, 3584], P(None, 'tensor', 'cand'), may hold values from -0.046875 to 0.046875
- pre_gain: float32 [3584], replicated, may hold values from 0.5 to 2
- post_gain: float32 [3584], replicated, may hold values from 0.5 to 2
- final_gain: float32 [3584], replicated, may hold values from 0.5 to 2
- unembed: bfloat16 [3584, 131072], P(None, ('cand', 'tensor')), may hold values from -0.3125 to 0.3125
Outputs:
- token_loss: float32 [512], P('cand')
- cand_loss: float32 [4], replicated
The draws below stay inside these ranges and needn't reach their ends.
All inputs are finite; a program needn't handle non-finite values. No bound on the sum of `loss_mask` on one device may be relied on, other than what follows from the above.
Results may differ from the reference program's by a relative error of at most 0.002.
Values may be sent and summed in bfloat16 or wider, within the bound.
No kernel may reach another device: no remote copies, remote signals or barrier semaphores. Data moves between devices by JAX's collectives and lax.ppermute only.
A program may use at most 128 MiB of HBM per device.

```python
import math
import jax
import jax.numpy as jnp
import numpy as np
from jax import lax

D = 3584
H = 16
KV = 8
HEAD_SIZE = 256
VOCAB = 131072
TASKS = 2
CANDS = 4
LENGTH = 128
TOKENS = 512
N_CAND = 4


def draw_states(key, part):
    first_key, second_key, third_key = jax.random.split(jax.random.fold_in(key, 11), 3)
    base = jax.random.normal(first_key, (TOKENS, D), jnp.float32)
    base = jnp.clip(base, -6.0, 6.0)
    row_scale = jnp.exp(jax.random.uniform(second_key, (TOKENS, 1), jnp.float32, 0.0, math.log(3.0)))
    column_scale = jnp.exp(jax.random.uniform(third_key, (1, D), jnp.float32, -0.5 * math.log(3.0), 0.5 * math.log(3.0)))
    return (base * row_scale * column_scale).astype(jnp.bfloat16)


def with_ends(array, rng, least, largest):
    extent = array.shape
    index_at = [jax.random.randint(jax.random.fold_in(rng, axis), (), 0, extent[axis]) for axis in range(len(extent))]
    array = array.at[tuple(index_at)].set(least)
    longest = extent.index(max(extent))
    index_at[longest] = (index_at[longest] + 1) % extent[longest]
    return array.at[tuple(index_at)].set(largest)


def levels(rng, dims, cuts, least, largest):
    gain = 1.0
    for position, blocks in cuts:
        draws = jax.random.uniform(jax.random.fold_in(jax.random.fold_in(rng, 6), position), (blocks,), jnp.float32, least / len(cuts), largest / len(cuts))
        gain = gain * jnp.repeat(jnp.exp(draws), dims[position] // blocks).reshape((-1,) + (1,) * (len(dims) - 1 - position))
    return gain


def skewed_wide(stream_key, shape, amount, skew):
    portions = [min(1 << octave, amount + 1 - (1 << octave)) * (1 << 20) // math.isqrt((1 << octave) ** skew) + 1 for octave in range((amount + 1).bit_length()) if 1 << octave <= amount]
    spread = 1 + sum(portions) // (1 << 30)
    table = np.cumsum(np.array([max(1, weight // spread) for weight in portions]))
    pick = jax.random.randint(jax.random.fold_in(stream_key, 1), shape, 0, int(table[len(portions) - 1]))
    start = jnp.left_shift(1, jnp.searchsorted(jnp.asarray(table, jnp.int32), pick, side="right").astype(jnp.int32))
    grade = start - 1 + jax.random.randint(jax.random.fold_in(stream_key, 4), shape, 0, 1 << 30) % jnp.minimum(start, amount + 1 - start)
    return jax.random.permutation(jax.random.fold_in(stream_key, 2), amount)[grade].astype(jnp.int32)


def centred(own_key, shape, width, bound, pieces=(), held_as=jnp.bfloat16):
    result = jax.random.normal(own_key, shape, jnp.float32) * width
    if len(pieces) > 0:
        result = levels(own_key, shape, pieces, -0.22, 0.18) * result
    return jnp.clip(result, min=-bound, max=bound).astype(held_as)


def setup_inputs(seed: int = 0) -> dict:
    seeds = jax.random.split(jax.random.key(seed), 18)
    return {
        "states": draw_states(jax.random.fold_in(seeds[17], 71), 0),
        "targets": with_ends(skewed_wide(seeds[1], (TOKENS,), VOCAB, 2), jax.random.fold_in(seeds[1], 3), 0, VOCAB - 1).astype(jnp.int32),
        "loss_mask": with_ends((jax.random.randint(seeds[2], (TOKENS,), 0, 4) < 3).astype(jnp.int32), jax.random.fold_in(seeds[2], 1), 0, 1),
        "cand_of": with_ends(jax.random.randint(seeds[3], (N_CAND,), 0, CANDS), jax.random.fold_in(seeds[3], 1), 0, CANDS - 1).astype(jnp.int32),
        "lambdas": jnp.clip(jax.random.uniform(seeds[4], (CANDS,), jnp.float32, 0.2, 1.0), 0.2, 1.0),
        "base_q": centred(seeds[5], (D, H * HEAD_SIZE), D ** -0.5, 0.09375, ((0, 4), (1, 8))),
        "delta_q": centred(seeds[6], (TASKS, D, H * HEAD_SIZE), (4 * D) ** -0.5, 0.046875, ((1, 4), (2, 8))),
        "base_k": centred(seeds[7], (D, KV * HEAD_SIZE), D ** -0.5, 0.09375, ((0, 4),)),
        "delta_k": centred(seeds[8], (TASKS, D, KV * HEAD_SIZE), (4 * D) ** -0.5, 0.046875, ((1, 4),)),
        "base_v": centred(seeds[9], (D, KV * HEAD_SIZE), D ** -0.5, 0.09375, ((0, 4),)),
        "delta_v": centred(seeds[10], (TASKS, D, KV * HEAD_SIZE), (4 * D) ** -0.5, 0.046875, ((1, 4),)),
        "base_o": centred(seeds[11], (H * HEAD_SIZE, D), (H * HEAD_SIZE) ** -0.5, 0.09375, ((0, 8), (1, 4))),
        "delta_o": centred(seeds[12], (TASKS, H * HEAD_SIZE, D), (4 * H * HEAD_SIZE) ** -0.5, 0.046875, ((1, 8), (2, 4))),
        "pre_gain": jnp.clip(jnp.exp(jax.random.uniform(seeds[13], (D,), jnp.float32, math.log(0.5), math.log(2.0))), 0.5, 2.0),
        "post_gain": jnp.clip(jnp.exp(jax.random.uniform(seeds[14], (D,), jnp.float32, math.log(0.5), math.log(2.0))), 0.5, 2.0),
        "final_gain": jnp.clip(jnp.exp(jax.random.uniform(seeds[15], (D,), jnp.float32, math.log(0.5), math.log(2.0))), 0.5, 2.0),
        "unembed": centred(seeds[16], (D, VOCAB), (D // 9) ** -0.5, 0.3125, ((1, 32),)),
    }


def root_norm(entries, scale_gain):
    mean_square = lax.optimization_barrier(jnp.mean(entries * entries, axis=-1, keepdims=True))
    return entries * lax.rsqrt(mean_square + 1e-06) * scale_gain

def rotate_pairs(entries, length):
    half_width = entries.shape[-1] // 2
    positions = jnp.arange(length).astype(jnp.float32)
    frequency = jnp.exp(-math.log(10000.0) * jnp.arange(half_width).astype(jnp.float32) * 2.0 / entries.shape[-1])
    angles = positions[:, None] * frequency[None, :]
    cosine = jnp.cos(angles)[:, None, :]
    sine_part = jnp.sin(angles)[:, None, :]
    first = entries[..., :half_width]
    second = entries[..., half_width:]
    return jnp.concatenate([first * cosine - second * sine_part, second * cosine + first * sine_part], axis=-1)

def merge_weights(base, total, mixing):
    return (base.astype(jnp.float32) + mixing * total.astype(jnp.float32)).astype(jnp.bfloat16)

def reference(states, targets, loss_mask, cand_of, lambdas, base_q, delta_q, base_k, delta_k, base_v, delta_v, base_o, delta_o, pre_gain, post_gain, final_gain, unembed):
    task_sums = [lax.optimization_barrier(jnp.sum(delta.astype(jnp.float32), axis=0)).astype(jnp.bfloat16) for delta in (delta_q, delta_k, delta_v, delta_o)]
    causal = jnp.arange(LENGTH)[:, None] >= jnp.arange(LENGTH)[None, :]

    def one_sequence(inputs):
        seq_states, seq_targets, seq_mask, mixing = inputs
        w_query = merge_weights(base_q, task_sums[0], mixing)
        w_key = merge_weights(base_k, task_sums[1], mixing)
        w_value = merge_weights(base_v, task_sums[2], mixing)
        w_out = merge_weights(base_o, task_sums[3], mixing)
        stream = seq_states.astype(jnp.float32)
        normed = root_norm(stream, pre_gain).astype(jnp.bfloat16)
        query_rows = jnp.dot(normed, w_query, preferred_element_type=jnp.float32).reshape(LENGTH, H, HEAD_SIZE)
        query_rows = rotate_pairs(query_rows, LENGTH).astype(jnp.bfloat16)
        key_proj = jnp.dot(normed, w_key, preferred_element_type=jnp.float32).astype(jnp.bfloat16).reshape(LENGTH, KV, HEAD_SIZE)
        value_proj = jnp.dot(normed, w_value, preferred_element_type=jnp.float32).astype(jnp.bfloat16).reshape(LENGTH, KV, HEAD_SIZE)
        key_matrix = rotate_pairs(key_proj.astype(jnp.float32), LENGTH).astype(jnp.bfloat16)
        key_matrix = jnp.repeat(key_matrix, H // KV, axis=1)
        value_matrix = jnp.repeat(value_proj, H // KV, axis=1)
        attention_scores = jnp.einsum('jfg,sfg->fjs', query_rows.astype(jnp.float32), key_matrix.astype(jnp.float32)) * HEAD_SIZE ** (-0.5)
        attention_scores = 50.0 * jnp.tanh(attention_scores / 50.0)
        weights = jnp.where(causal[None, :, :], jnp.exp(attention_scores), 0.0)
        attention_probs = (weights / lax.optimization_barrier(jnp.sum(weights, axis=-1, keepdims=True))).astype(jnp.bfloat16)
        context_rows = jnp.einsum('pvs,spt->vpt', attention_probs.astype(jnp.float32), value_matrix.astype(jnp.float32))
        context_rows = context_rows.astype(jnp.bfloat16).reshape(LENGTH, H * HEAD_SIZE)
        attended = jnp.dot(context_rows, w_out, preferred_element_type=jnp.float32)
        mixed = stream + root_norm(attended, post_gain)
        final_rows = root_norm(mixed, final_gain).astype(jnp.bfloat16)
        logits = jnp.dot(final_rows, unembed, preferred_element_type=jnp.float32)
        capped = 30.0 * jnp.tanh(logits / 30.0)
        totals = lax.optimization_barrier(jnp.sum(jnp.exp(capped), axis=-1))
        picked = jnp.take_along_axis(capped, seq_targets[:, None].astype(jnp.int32), axis=1)[:, 0]
        return seq_mask.astype(jnp.float32) * (jnp.log(totals) - picked)
    losses = lax.map(one_sequence, (states.reshape(N_CAND, LENGTH, D), targets.reshape(N_CAND, LENGTH), loss_mask.reshape(N_CAND, LENGTH), lambdas[cand_of]))
    onehot = (cand_of[:, None] == jnp.arange(CANDS)[None, :]).astype(jnp.float32)
    seq_sums = lax.optimization_barrier(jnp.sum(losses, axis=1))
    seq_counts = lax.optimization_barrier(jnp.sum(loss_mask.reshape(N_CAND, LENGTH).astype(jnp.float32), axis=1))
    loss_sums = lax.optimization_barrier(jnp.sum(onehot * seq_sums[:, None], axis=0))
    counts = lax.optimization_barrier(jnp.sum(onehot * seq_counts[:, None], axis=0))
    return (losses.reshape(TOKENS), loss_sums / jnp.maximum(counts, 1.0))
```

```python
import functools
import math

import jax
import jax.numpy as jnp
from jax import lax
from jax.experimental import pallas as pl
from jax.experimental.pallas import tpu as pltpu
from jax.sharding import PartitionSpec as P

KV = 8
HEAD_SIZE = 256
CANDS = 4
EPS = 1e-06
BF16 = jnp.bfloat16
F32 = jnp.float32
PARTS = 2
MIB = 1024 * 1024

VM = pl.BlockSpec(memory_space=pltpu.VMEM)
SM = pl.BlockSpec(memory_space=pltpu.SMEM)


def params(mib):
    return pltpu.CompilerParams(vmem_limit_bytes=mib * MIB)


def cost(flops, nbytes):
    return pl.CostEstimate(flops=int(flops), bytes_accessed=int(nbytes), transcendentals=0)


def shape(dims, dtype):
    return jax.ShapeDtypeStruct(tuple(dims), dtype)


def swap(value, axis, mask):
    size = lax.axis_size(axis)
    return lax.ppermute(value, axis, [(i, i ^ mask) for i in range(size)])


def swap_both(value, cand_mask, tensor_mask):
    cands, tensors = lax.axis_size("cand"), lax.axis_size("tensor")
    pairs = [
        (c * tensors + t, (c ^ cand_mask) * tensors + (t ^ tensor_mask))
        for c in range(cands)
        for t in range(tensors)
    ]
    return lax.ppermute(value, ("cand", "tensor"), pairs)


def tile_of(size, *choices):
    for choice in choices:
        if size % choice == 0:
            return choice
    return size


TAIL = 8


def cut_body(width, ids, states, *pieces):
    length = states.shape[0]
    stream = states[...].astype(F32)
    mean = jnp.mean(stream * stream, axis=-1, keepdims=True)
    rest = jnp.transpose(jnp.broadcast_to(lax.rsqrt(mean + EPS), (length, 128)))[:TAIL]
    rows = lax.broadcasted_iota(jnp.int32, (TAIL, length), 0)
    tail = jnp.zeros((TAIL, length), F32)
    for row in range(3):
        term = rest.astype(BF16).astype(F32)
        tail = jnp.where(rows == row, term, tail)
        rest = rest - term
    tail = tail.astype(BF16)
    for k, out in enumerate(pieces):
        start = pl.multiple_of((ids[0] ^ k) * width, 128)
        out[:length, :] = states[:, pl.ds(start, width)]
        out[length:, :] = jnp.zeros((TAIL, width), BF16)
        out[length:, :length] = tail


def cut_call(ids, states, cands):
    length, features = states.shape
    width = features // cands
    return pl.pallas_call(
        functools.partial(cut_body, width),
        in_specs=[SM, VM],
        out_specs=[VM] * cands,
        out_shape=[shape((length + TAIL, width), BF16)] * cands,
        compiler_params=params(8),
        cost_estimate=cost(1e9, 4 * states.size),
        name="cut",
    )(ids, states)


def cut_plain(own, states, cands):
    length, features = states.shape
    width = features // cands
    stream = states.astype(F32)
    rest = lax.rsqrt(jnp.mean(stream * stream, axis=-1) + EPS)
    terms = []
    for _ in range(3):
        term = lax.reduce_precision(rest, 8, 7)
        terms.append(term)
        rest = rest - term
    tail = jnp.pad(jnp.stack(terms), ((0, TAIL - 3), (0, width - length))).astype(BF16)
    return [
        jnp.concatenate(
            [lax.dynamic_slice_in_dim(states, (own ^ k) * width, width, 1), tail], axis=0
        )
        for k in range(cands)
    ]


def task_sum(delta):
    total = delta[0].astype(F32)
    for task in range(1, delta.shape[0]):
        total = total + delta[task].astype(F32)
    return total.astype(BF16)


def prep_body(ids, *refs):
    *ins, out = refs
    half = out.shape[1] // 2
    col = 0
    for base, delta in zip(ins[::2], ins[1::2]):
        width = base.shape[1]
        out[:, col : col + width] = base[...]
        out[:, half + col : half + col + width] = task_sum(delta)
        col += width


def prep_call(ids, pairs):
    rows = pairs[0][0].shape[0]
    tile = tile_of(rows, 128, 112, 64, 32, 16)
    specs, operands, total_width = [], [], 0
    for base, delta, width, of_head in pairs:
        at = (lambda ids: ids[1]) if of_head else (lambda ids: 0)
        specs.append(pl.BlockSpec((tile, width), lambda i, ids, at=at: (i, at(ids))))
        specs.append(
            pl.BlockSpec((delta.shape[0], tile, width), lambda i, ids, at=at: (0, i, at(ids)))
        )
        operands += [base, delta]
        total_width += width
    return pl.pallas_call(
        prep_body,
        grid_spec=pltpu.PrefetchScalarGridSpec(
            num_scalar_prefetch=1,
            grid=(rows // tile,),
            in_specs=specs,
            out_specs=pl.BlockSpec((tile, 2 * total_width), lambda i, ids: (i, 0)),
        ),
        out_shape=shape((rows, 2 * total_width), BF16),
        compiler_params=params(58),
        cost_estimate=cost(2e9, rows * total_width * 10),
        name="prep",
    )(ids, *operands)


def qkv_body(count, first, ids, cand_of, lambdas, *refs):
    pieces, gain, weights = refs[:count], refs[count], refs[count + 1]
    outs, normed = refs[count + 2 : -1], refs[-1]
    length, columns = outs[0].shape
    for k in range(count):
        turned = jnp.transpose(pieces[k][length:, :length].astype(F32))
        column = turned[:, 0:1] + turned[:, 1:2] + turned[:, 2:3]
        raw = pieces[k][:length, :].astype(F32)
        normed[k * length : (k + 1) * length, :] = (raw * column * gain[...][:1]).astype(BF16)
    chunk = tile_of(columns, 256, 128)
    for start in range(0, columns, chunk):
        base = jnp.dot(
            normed[...], weights[:, start : start + chunk], preferred_element_type=F32
        )
        task = jnp.dot(
            normed[...],
            weights[:, columns + start : columns + start + chunk],
            preferred_element_type=F32,
        )
        for k in range(count):
            mixing = lambdas[cand_of[ids[0] ^ (first + k)]]
            rows = slice(k * length, (k + 1) * length)
            outs[k][:, start : start + chunk] = base[rows] + mixing * task[rows]


def qkv_call(ids, cand_of, lambdas, pieces, gain, weights, first):
    count = len(pieces)
    length, width = pieces[0].shape[0] - TAIL, pieces[0].shape[1]
    columns = weights.shape[1] // 2
    return pl.pallas_call(
        functools.partial(qkv_body, count, first),
        in_specs=[SM] * 3 + [VM] * (count + 2),
        out_specs=[VM] * count,
        out_shape=[shape((length, columns), F32)] * count,
        scratch_shapes=[pltpu.VMEM((count * length, width), BF16)],
        compiler_params=params(16),
        cost_estimate=cost(4 * count * length * width * columns, 2 * weights.size),
        name="qkv",
    )(ids, cand_of, lambdas, *pieces, gain, weights)


def join_body(own, other, out):
    out[...] = (own[...] + other[...]).astype(BF16)


def join_call(own, other):
    return pl.pallas_call(
        join_body,
        in_specs=[VM, VM],
        out_specs=VM,
        out_shape=shape(own.shape, BF16),
        compiler_params=params(4),
        cost_estimate=cost(1e8, 10 * own.size),
        name="join",
    )(own, other)


def attend_body(n_more, heads, *refs):
    own, cosine, sine = refs[:3]
    more, out = refs[3 : 3 + n_more], refs[3 + n_more]
    length = own.shape[0]
    half = HEAD_SIZE // 2
    cos, sin = cosine[...], sine[...]

    def piece(start, width):
        total = own[:, start : start + width]
        for ref in more:
            total = total + ref[:, start : start + width].astype(F32)
        return total

    def rotate(u):
        first, second = u[:, :half], u[:, half:]
        return jnp.concatenate([first * cos - second * sin, second * cos + first * sin], axis=-1)

    q_width = heads * HEAD_SIZE
    key = rotate(piece(q_width, HEAD_SIZE).astype(BF16).astype(F32)).astype(BF16)
    value = piece(q_width + HEAD_SIZE, HEAD_SIZE).astype(BF16)
    rows = lax.broadcasted_iota(jnp.int32, (length, length), 0)
    columns = lax.broadcasted_iota(jnp.int32, (length, length), 1)
    causal = rows >= columns
    for head in range(heads):
        query = rotate(piece(head * HEAD_SIZE, HEAD_SIZE)).astype(BF16)
        score = lax.dot_general(
            query, key, (((1,), (1,)), ((), ())), preferred_element_type=F32
        ) * HEAD_SIZE ** (-0.5)
        score = 50.0 * jnp.tanh(score / 50.0)
        weight = jnp.where(causal, jnp.exp(score), 0.0)
        probs = (weight / jnp.sum(weight, axis=-1, keepdims=True)).astype(BF16)
        context = jnp.dot(probs, value, preferred_element_type=F32)
        out[:, head * HEAD_SIZE : (head + 1) * HEAD_SIZE] = context.astype(BF16)


def attend_call(own, more, cosine, sine, heads):
    length = own.shape[0]
    return pl.pallas_call(
        functools.partial(attend_body, len(more), heads),
        in_specs=[VM] * (3 + len(more)),
        out_specs=VM,
        out_shape=shape((length, heads * HEAD_SIZE), BF16),
        compiler_params=params(16),
        cost_estimate=cost(1e9, 4 * own.size),
        name="attend",
    )(own, cosine, sine, *more)


def project_body(cands, group, ids, cand_of, lambdas, *refs):
    contexts, base, task = refs[:cands], refs[cands], refs[cands + 1]
    keep, send, stack = refs[cands + 2 :]
    own, bit = ids[0], ids[1]
    half = group // 2
    length, width = keep.shape[1:]
    for k in range(cands):
        stack[k * length : (k + 1) * length, :] = contexts[k][...]
    for start in range(0, width, 256):
        cols = slice(start, min(start + 256, width))
        of_base = jnp.dot(stack[...], base[:, cols], preferred_element_type=F32)
        of_task = jnp.dot(stack[...], task[:, cols], preferred_element_type=F32)
        for k in range(cands):
            seq = own ^ k
            part, inside = seq // group, seq % group
            at = part * half + inside % half
            mixing = lambdas[cand_of[seq]]
            rows = slice(k * length, (k + 1) * length)
            result = of_base[rows] + mixing * of_task[rows]
            mine = inside // half == bit

            @pl.when(mine)
            def _():
                keep[at, :, cols] = result

            @pl.when(jnp.logical_not(mine))
            def _():
                send[at, :, cols] = result.astype(BF16)


def project_call(ids, cand_of, lambdas, contexts, base, task, group):
    cands = len(contexts)
    length, depth = contexts[0].shape
    width = base.shape[1]
    return pl.pallas_call(
        functools.partial(project_body, cands, group),
        in_specs=[SM] * 3 + [VM] * (cands + 2),
        out_specs=[VM, VM],
        out_shape=[shape((cands // 2, length, width), F32), shape((cands // 2, length, width), BF16)],
        scratch_shapes=[pltpu.VMEM((cands * length, depth), BF16)],
        compiler_params=params(24),
        cost_estimate=cost(4 * cands * length * width * depth, 4 * base.size),
        name="project",
    )(ids, cand_of, lambdas, *contexts, base, task)


def tasks_body(delta, out):
    out[...] = task_sum(delta)


def tasks_call(delta):
    tasks, rows, width = delta.shape
    tile = tile_of(rows, 128)
    return pl.pallas_call(
        tasks_body,
        grid=(rows // tile,),
        in_specs=[pl.BlockSpec((tasks, tile, width), lambda i: (0, i, 0))],
        out_specs=pl.BlockSpec((tile, width), lambda i: (i, 0)),
        out_shape=shape((rows, width), BF16),
        compiler_params=params(16),
        cost_estimate=cost(1e9, 6 * rows * width),
        name="tasks",
    )(delta)


def spread_body(blocks, rows, ids, keep, got, own, *sends):
    at = ids[2]
    for mask in range(blocks):
        start = pl.multiple_of((at ^ mask) * rows, rows)
        total = keep[pl.ds(start, rows), :] + got[pl.ds(start, rows), :].astype(F32)
        if mask == 0:
            own[...] = total
        else:
            sends[mask - 1][...] = total.astype(BF16)


def spread_call(ids, keep, got, blocks):
    rows, width = keep.shape[0] // blocks, keep.shape[1]
    return pl.pallas_call(
        functools.partial(spread_body, blocks, rows),
        in_specs=[SM, VM, VM],
        out_specs=[VM] * blocks,
        out_shape=[shape((rows, width), F32)] + [shape((rows, width), BF16)] * (blocks - 1),
        compiler_params=params(8),
        cost_estimate=cost(1e9, 8 * keep.size),
        name="spread",
    )(ids, keep, got)


def sums_body(n_got, n_raw, rows, ids, own, gain, *refs):
    got, raw = refs[:n_got], refs[n_got : n_got + n_raw]
    attended, stream, sums = refs[n_got + n_raw :]
    a = own[...]
    for ref in got:
        a = a + ref[...].astype(F32)
    attended[...] = a
    take = min(rows, raw[0].shape[0] - TAIL)
    for step in range(rows // take):
        for k in range(n_raw):

            @pl.when(ids[step] == k)
            def _():
                start = pl.multiple_of(ids[rows // take], take)
                stream[step * take : (step + 1) * take, :] = raw[k][pl.ds(start, take), :]

    s = stream[...].astype(F32)
    ag = a * gain[...][:1]
    lanes = lax.broadcasted_iota(jnp.int32, sums.shape, 1)
    total = jnp.zeros(sums.shape, F32)
    for lane, term in enumerate((a * a, s * s, s * ag, ag * ag)):
        total = jnp.where(lanes == lane, jnp.sum(term, axis=1, keepdims=True), total)
    sums[...] = total


def sums_call(ids, own, got, raw, gain):
    rows, width = own.shape
    return pl.pallas_call(
        functools.partial(sums_body, len(got), len(raw), rows),
        in_specs=[SM] + [VM] * (2 + len(got) + len(raw)),
        out_specs=[VM] * 3,
        out_shape=[shape((rows, width), F32), shape((rows, width), BF16), shape((rows, 128), F32)],
        compiler_params=params(8),
        cost_estimate=cost(1e9, 8 * own.size),
        name="sums",
    )(ids, own, gain, *got, *raw)


def finish_body(features, n_sums, attended, stream, post, final, *refs):
    sums, out = refs[:n_sums], refs[n_sums]
    total = sums[0][...]
    for ref in sums[1:]:
        total = total + ref[...]
    aa, ss, sag, agag = (total[:, i : i + 1] / features for i in range(4))
    first = lax.rsqrt(aa + EPS)
    second = lax.rsqrt(ss + 2.0 * first * sag + first * first * agag + EPS)
    mixed = stream[...].astype(F32) + attended[...] * first * post[...][:1]
    out[...] = (mixed * second * final[...][:1]).astype(BF16)


def finish_call(attended, stream, post, final, sums, features):
    return pl.pallas_call(
        functools.partial(finish_body, features, len(sums)),
        in_specs=[VM] * (4 + len(sums)),
        out_specs=VM,
        out_shape=shape(attended.shape, BF16),
        compiler_params=params(8),
        cost_estimate=cost(1e9, 8 * attended.size),
        name="finish",
    )(attended, stream, post, final, *sums)


def vocab_body(n_pieces, blocks, rows, width, at, targets, *refs):
    pieces = refs[:n_pieces]
    unembed, out, x, sem, acc = refs[n_pieces : n_pieces + 5]
    step = pl.program_id(0)

    def copies():
        for p in range(n_pieces):
            for m in range(blocks):
                row = pl.multiple_of(at[p * (blocks + 1) + 1 + m] * rows, rows)
                col = pl.multiple_of(at[p * (blocks + 1)] * width, 128)
                yield pltpu.make_async_copy(
                    pieces[p].at[pl.ds(m * rows, rows), :],
                    x.at[pl.ds(row, rows), pl.ds(col, width)],
                    sem.at[p * blocks + m],
                )

    @pl.when(step == 0)
    def _():
        for copy in copies():
            copy.start()
        acc[...] = jnp.zeros_like(acc)
        for copy in copies():
            copy.wait()

    vocab_tile(step, targets, x, unembed, out, acc)


def vocab_tile(step, targets, x, unembed, out, acc):
    rows, tile = x.shape[0], unembed.shape[1]
    sub = tile_of(tile, 256, 128)
    local = targets[...] - step * tile
    columns = lax.broadcasted_iota(jnp.int32, (rows, 128), 1)
    totals = jnp.zeros((rows, 128), F32)
    picked = jnp.zeros((rows, 128), F32)
    for start in range(0, tile, sub):
        logits = jnp.dot(
            x[...], unembed[:, start : start + sub], preferred_element_type=F32
        )
        for lane in range(0, sub, 128):
            capped = 30.0 * jnp.tanh(logits[:, lane : lane + 128] / 30.0)
            totals += jnp.exp(capped)
            picked += jnp.where(columns == local - (start + lane), capped, 0.0)
    acc[:, :128] += totals
    acc[:, 128:] += picked

    @pl.when(step == pl.num_programs(0) - 1)
    def _():
        for row in range(2):
            turned = jnp.transpose(acc[:, row * 128 : (row + 1) * 128])
            out[row : row + 1, :] = jnp.sum(turned, axis=0, keepdims=True)


def vocab_plain_body(targets, x, unembed, out, acc):
    step = pl.program_id(0)

    @pl.when(step == 0)
    def _():
        acc[...] = jnp.zeros_like(acc)

    vocab_tile(step, targets, x, unembed, out, acc)


def vocab_call(pieces, places, targets, unembed, blocks):
    rows, width = pieces[0].shape[0] // blocks, pieces[0].shape[1]
    total_rows = targets.shape[0]
    features, vocab = unembed.shape
    tile = tile_of(vocab, 1024, 512, 256, 128)
    spec = dict(
        out_shape=shape((8, total_rows), F32),
        compiler_params=params(40),
        cost_estimate=cost(2 * total_rows * features * vocab, 2 * unembed.size),
        name="vocab",
    )
    if width % 128 == 0:
        full = pl.BlockSpec((8, total_rows), lambda i, *_: (0, 0))
        return pl.pallas_call(
            functools.partial(vocab_body, len(pieces), blocks, rows, width),
            grid_spec=pltpu.PrefetchScalarGridSpec(
                num_scalar_prefetch=1,
                grid=(vocab // tile,),
                in_specs=[pl.BlockSpec((total_rows, 1), lambda i, *_: (0, 0))]
                + [pl.BlockSpec(memory_space=pl.ANY)] * len(pieces)
                + [pl.BlockSpec((features, tile), lambda i, *_: (0, i))],
                out_specs=full,
                scratch_shapes=[
                    pltpu.VMEM((total_rows, features), BF16),
                    pltpu.SemaphoreType.DMA((len(pieces) * blocks,)),
                    pltpu.VMEM((total_rows, 256), F32),
                ],
            ),
            **spec,
        )(jnp.concatenate(places).astype(jnp.int32), targets, *pieces, unembed)
    x = jnp.zeros((total_rows, features), BF16)
    for piece, place in zip(pieces, places):
        for m in range(blocks):
            x = lax.dynamic_update_slice(
                x, piece[m * rows : (m + 1) * rows], (place[1 + m] * rows, place[0] * width)
            )
    return pl.pallas_call(
        vocab_plain_body,
        grid=(vocab // tile,),
        in_specs=[
            pl.BlockSpec((total_rows, 1), lambda i: (0, 0)),
            pl.BlockSpec((total_rows, features), lambda i: (0, 0)),
            pl.BlockSpec((features, tile), lambda i: (0, i)),
        ],
        out_specs=pl.BlockSpec((8, total_rows), lambda i: (0, 0)),
        scratch_shapes=[pltpu.VMEM((total_rows, 256), F32)],
        **spec,
    )(targets, x, unembed)


def on_device(
    states,
    targets,
    loss_mask,
    cand_of,
    lambdas,
    base_q,
    delta_q,
    base_k,
    delta_k,
    base_v,
    delta_v,
    base_o,
    delta_o,
    pre_gain,
    post_gain,
    final_gain,
    unembed,
):
    cands, tensors = lax.axis_size("cand"), lax.axis_size("tensor")
    own, place = lax.axis_index("cand"), lax.axis_index("tensor")
    length, features = states.shape
    width = features // cands
    tokens = cands * length
    heads = base_q.shape[1] // HEAD_SIZE
    blocks = tensors // 2
    bit, block = place % 2, place // 2
    head = place // (tensors // KV)

    ids = jnp.stack([own, head]).astype(jnp.int32)
    aligned = width % 128 == 0 and length == 128
    cuts = cut_call(ids, states, cands) if aligned else cut_plain(own, states, cands)
    xs = [cuts[0]] + [None] * (cands - 1)
    for k in [*range(2, cands), 1]:
        xs[k] = swap(cuts[k], "cand", k)

    weights = prep_call(
        ids,
        [
            (base_q, delta_q, base_q.shape[1], False),
            (base_k, delta_k, HEAD_SIZE, True),
            (base_v, delta_v, HEAD_SIZE, True),
        ],
    )
    task_o = tasks_call(delta_o)

    gains = jnp.stack([pre_gain, post_gain, final_gain])
    gains = lax.dynamic_slice_in_dim(gains, own * width, width, 1)
    gain, post, final = (jnp.broadcast_to(gains[i : i + 1], (8, width)) for i in range(3))
    partials = []
    for first in range(0, cands, 2):
        partials += qkv_call(
            ids, cand_of, lambdas, xs[first : first + 2], gain, weights, first
        )
    crossed = [swap(partials[k + 1], "cand", 1) for k in range(0, cands, 2)]
    more = [crossed[0]]
    for k in range(2, cands, 2):
        more.append(swap(join_call(partials[k], crossed[k // 2]), "cand", k))

    positions = jnp.arange(length).astype(F32)
    half = HEAD_SIZE // 2
    frequency = jnp.exp(-math.log(10000.0) * jnp.arange(half).astype(F32) * 2.0 / HEAD_SIZE)
    angles = positions[:, None] * frequency[None, :]
    context = attend_call(partials[0], more, jnp.cos(angles), jnp.sin(angles), heads)

    contexts = [None] * cands
    contexts[0] = context
    for k in range(2, cands, 2):
        contexts[k] = swap(context, "cand", k)
    for k in range(0, cands, 2):
        contexts[k + 1] = swap(contexts[k], "cand", 1)

    group = cands // PARTS
    keep, send = project_call(
        jnp.stack([own, bit]).astype(jnp.int32), cand_of, lambdas, contexts, base_o, task_o, group
    )
    part_rows = tokens // PARTS
    rows = part_rows // tensors
    spot = jnp.stack([own, bit, block]).astype(jnp.int32)
    arrived, results = [], []
    for part in range(PARTS):
        lo, hi = part * group // 2, (part + 1) * group // 2
        got = swap(send[lo:hi], "tensor", 1).reshape(part_rows // 2, width)
        mine, *sends = spread_call(spot, keep[lo:hi].reshape(part_rows // 2, width), got, blocks)
        got = [swap(sends[m - 1], "tensor", 2 * m) for m in range(1, blocks)]
        first_row = part * part_rows + (bit * blocks + block) * rows
        where = jnp.stack(
            [(first_row // length + i) ^ own for i in range(max(1, rows // length))]
            + [first_row % length]
        ).astype(jnp.int32)
        attended, s, sums = sums_call(where, mine, got, xs, post)
        every = [sums] + [swap(sums, "cand", k) for k in range(1, cands)]
        final_rows = finish_call(attended, s, post, final, every, features)
        pile = [final_rows] + [swap(final_rows, "tensor", 2 * m) for m in range(1, blocks)]
        pile = jnp.concatenate(pile, axis=0)
        crossing = []
        for cand_mask in range(0, cands, 2):
            for bit_mask in range(2):
                moved = cand_mask or bit_mask
                crossing.append(swap_both(pile, cand_mask, bit_mask) if moved else pile)
        arrived.append(crossing)
    for part in range(PARTS):
        crossing = arrived[part]
        if part > 0:
            crossing, results[-1] = lax.optimization_barrier((crossing, results[-1]))
        pieces, places = [], []
        for index, piece in enumerate(crossing):
            cand_mask, bit_mask = index // 2 * 2, index % 2
            for core_mask in range(2):
                pieces.append(swap(piece, "cand", 1) if core_mask else piece)
                places.append(
                    jnp.stack(
                        [own ^ cand_mask ^ core_mask]
                        + [(bit ^ bit_mask) * blocks + (block ^ m) for m in range(blocks)]
                    )
                )
        vocab_start = (own * tensors + place) * unembed.shape[1]
        ids_here = targets[part * part_rows : (part + 1) * part_rows] - vocab_start
        results.append(
            vocab_call(pieces, places, ids_here.reshape(part_rows, 1), unembed, blocks)
        )
    both = jnp.concatenate(results, axis=1)[:2]
    masks = jnp.where(
        (lax.broadcasted_iota(jnp.int32, (cands, 1), 0) == own) & (place == 0),
        loss_mask.astype(F32)[None, :],
        0.0,
    ).reshape(1, tokens)
    payload = jnp.concatenate([both, masks], axis=0)
    payload = jnp.broadcast_to(payload[None], (cands * tensors,) + payload.shape)
    summed = jnp.sum(lax.all_to_all(payload, ("cand", "tensor"), 0, 0), axis=0)
    mask_values = summed[2]
    losses = mask_values * (jnp.log(summed[0]) - summed[1])
    token_loss = lax.dynamic_slice_in_dim(losses, own * length, length, 0)
    onehot = (cand_of[:, None] == jnp.arange(CANDS)[None, :]).astype(F32)
    loss_sums = jnp.sum(onehot * jnp.sum(losses.reshape(cands, length), axis=1)[:, None], axis=0)
    counts = jnp.sum(onehot * jnp.sum(mask_values.reshape(cands, length), axis=1)[:, None], axis=0)
    return (token_loss, loss_sums / jnp.maximum(counts, 1.0))


def solution(mesh):
    in_specs = (
        P("cand", None),
        P(),
        P("cand"),
        P(),
        P(),
        P("cand", "tensor"),
        P(None, "cand", "tensor"),
        P("cand", None),
        P(None, "cand", None),
        P("cand", None),
        P(None, "cand", None),
        P("tensor", "cand"),
        P(None, "tensor", "cand"),
        P(),
        P(),
        P(),
        P(None, ("cand", "tensor")),
    )
    out_specs = (P("cand"), P())
    return jax.shard_map(
        on_device, mesh=mesh, in_specs=in_specs, out_specs=out_specs, check_vma=False
    )
```

```python
import functools
import math

import jax
import jax.numpy as jnp
from jax import lax
from jax.experimental import pallas as pl
from jax.experimental.pallas import tpu as pltpu
from jax.sharding import PartitionSpec as P


KV = 8
HEAD_SIZE = 256
CANDS = 4
EPS = 1e-06
BF16 = jnp.bfloat16
F32 = jnp.float32
PARTS = 2
MIB = 1024 * 1024

VM = pl.BlockSpec(memory_space=pltpu.VMEM)
SM = pl.BlockSpec(memory_space=pltpu.SMEM)
FAR = pl.BlockSpec(memory_space=pl.ANY)


def params(mib):
    return pltpu.CompilerParams(vmem_limit_bytes=mib * MIB)


def cost(flops, nbytes):
    return pl.CostEstimate(flops=int(flops), bytes_accessed=int(nbytes), transcendentals=0)


def shape(dims, dtype):
    return jax.ShapeDtypeStruct(tuple(dims), dtype)


def swap(value, axis, mask):
    size = lax.axis_size(axis)
    return lax.ppermute(value, axis, [(i, i ^ mask) for i in range(size)])


def swap_both(value, cand_mask, tensor_mask):
    cands, tensors = lax.axis_size("cand"), lax.axis_size("tensor")
    pairs = [
        (c * tensors + t, (c ^ cand_mask) * tensors + (t ^ tensor_mask))
        for c in range(cands)
        for t in range(tensors)
    ]
    return lax.ppermute(value, ("cand", "tensor"), pairs)


def tile_of(size, *choices):
    for choice in choices:
        if size % choice == 0:
            return choice
    return size


TAIL = 8


def cut_body(width, ids, states, *pieces):
    length = states.shape[0]
    stream = states[...].astype(F32)
    mean = jnp.mean(stream * stream, axis=-1, keepdims=True)
    rest = jnp.transpose(jnp.broadcast_to(lax.rsqrt(mean + EPS), (length, 128)))[:TAIL]
    rows = lax.broadcasted_iota(jnp.int32, (TAIL, length), 0)
    tail = jnp.zeros((TAIL, length), F32)
    for row in range(3):
        term = rest.astype(BF16).astype(F32)
        tail = jnp.where(rows == row, term, tail)
        rest = rest - term
    tail = tail.astype(BF16)
    for k, out in enumerate(pieces):
        start = pl.multiple_of((ids[0] ^ k) * width, 128)
        out[:length, :] = states[:, pl.ds(start, width)]
        out[length:, :] = jnp.zeros((TAIL, width), BF16)
        out[length:, :length] = tail


def cut_call(ids, states, cands):
    length, features = states.shape
    width = features // cands
    return pl.pallas_call(
        functools.partial(cut_body, width),
        in_specs=[SM, VM],
        out_specs=[VM] * cands,
        out_shape=[shape((length + TAIL, width), BF16)] * cands,
        compiler_params=params(8),
        cost_estimate=cost(1e9, 4 * states.size),
        name="cut",
    )(ids, states)


def cut_plain(own, states, cands):
    length, features = states.shape
    width = features // cands
    stream = states.astype(F32)
    rest = lax.rsqrt(jnp.mean(stream * stream, axis=-1) + EPS)
    terms = []
    for _ in range(3):
        term = lax.reduce_precision(rest, 8, 7)
        terms.append(term)
        rest = rest - term
    tail = jnp.pad(jnp.stack(terms), ((0, TAIL - 3), (0, width - length))).astype(BF16)
    return [
        jnp.concatenate(
            [lax.dynamic_slice_in_dim(states, (own ^ k) * width, width, 1), tail], axis=0
        )
        for k in range(cands)
    ]


def task_sum(delta):
    total = delta[0].astype(F32)
    for task in range(1, delta.shape[0]):
        total = total + delta[task].astype(F32)
    return total.astype(BF16)


def prep_body(ids, *refs):
    *ins, delta_o, out, out_o = refs
    delta_q, *ins = ins
    col = 0
    for base in ins[::2]:
        out[:, col : col + base.shape[1]] = base[...]
        col += base.shape[1]
    for delta in [delta_q, *ins[1::2]]:
        out[:, col : col + delta.shape[2]] = task_sum(delta)
        col += delta.shape[2]
    out_o[...] = task_sum(delta_o)


def prep_call(ids, delta_q, pairs, delta_o):
    rows = pairs[0][0].shape[0]
    width_q = delta_q.shape[2]
    tasks, rows_o, width_o = delta_o.shape
    steps = 1
    for choice in (2, 4, 8):
        if rows % (16 * choice) == 0 and rows_o % (16 * choice) == 0:
            steps = choice
    tile, tile_o = rows // steps, rows_o // steps
    specs = [pl.BlockSpec((tasks, tile, width_q), lambda i, ids: (0, i, 0))]
    operands, total_width = [delta_q], width_q
    for base, delta in pairs:
        specs.append(pl.BlockSpec((tile, HEAD_SIZE), lambda i, ids: (i, ids[1])))
        specs.append(pl.BlockSpec((tasks, tile, HEAD_SIZE), lambda i, ids: (0, i, ids[1])))
        operands += [base, delta]
        total_width += 2 * HEAD_SIZE
    specs.append(pl.BlockSpec((tasks, tile_o, width_o), lambda i, ids: (0, i, 0)))
    return pl.pallas_call(
        prep_body,
        grid_spec=pltpu.PrefetchScalarGridSpec(
            num_scalar_prefetch=1,
            grid=(steps,),
            in_specs=specs,
            out_specs=[
                pl.BlockSpec((tile, total_width), lambda i, ids: (i, 0)),
                pl.BlockSpec((tile_o, width_o), lambda i, ids: (i, 0)),
            ],
        ),
        out_shape=[shape((rows, total_width), BF16), shape((rows_o, width_o), BF16)],
        compiler_params=params(58),
        cost_estimate=cost(2e9, rows * total_width * 10),
        name="prep",
    )(ids, *operands, delta_o)


def qkv_body(count, first, ids, cand_of, lambdas, *refs):
    pieces, gain, base_q, weights = refs[:count], refs[count], refs[count + 1], refs[count + 2]
    outs, normed = refs[-1 - count : -1], refs[-1]
    width_q = base_q.shape[1]
    rest = outs[0].shape[1] - width_q
    length, columns = outs[0].shape
    for k in range(count):
        turned = jnp.transpose(pieces[k][length:, :length].astype(F32))
        column = turned[:, 0:1] + turned[:, 1:2] + turned[:, 2:3]
        raw = pieces[k][:length, :].astype(F32)
        normed[k * length : (k + 1) * length, :] = (raw * column * gain[...][:1]).astype(BF16)
    chunk = tile_of(columns, 256, 128)
    for start in range(0, columns, chunk):
        if start < width_q:
            first_term = base_q[:, start : start + chunk]
        else:
            first_term = weights[:, start - width_q : start - width_q + chunk]
        base = jnp.dot(normed[...], first_term, preferred_element_type=F32)
        task = jnp.dot(
            normed[...],
            weights[:, rest + start : rest + start + chunk],
            preferred_element_type=F32,
        )
        for k in range(count):
            mixing = lambdas[cand_of[ids[0] ^ (first + k)]]
            rows = slice(k * length, (k + 1) * length)
            outs[k][:, start : start + chunk] = base[rows] + mixing * task[rows]


def qkv_call(ids, cand_of, lambdas, pieces, gain, base_q, weights, first, after):
    count = len(pieces)
    length, width = pieces[0].shape[0] - TAIL, pieces[0].shape[1]
    columns = (weights.shape[1] + base_q.shape[1]) // 2
    return pl.pallas_call(
        functools.partial(qkv_body, count, first),
        in_specs=[SM] * 3 + [VM] * (count + 3) + [FAR] * len(after),
        out_specs=[VM] * count,
        out_shape=[shape((length, columns), F32)] * count,
        scratch_shapes=[pltpu.VMEM((count * length, width), BF16)],
        compiler_params=params(16),
        cost_estimate=cost(4 * count * length * width * columns, 2 * weights.size),
        name="qkv",
    )(ids, cand_of, lambdas, *pieces, gain, base_q, weights, *after)


def join_body(own, other, out):
    out[...] = (own[...] + other[...]).astype(out.dtype)


def join_call(own, other, dtype):
    return pl.pallas_call(
        join_body,
        in_specs=[VM, VM],
        out_specs=VM,
        out_shape=shape(own.shape, dtype),
        compiler_params=params(4),
        cost_estimate=cost(1e8, 10 * own.size),
        name="join",
    )(own, other)


def attend_body(n_more, heads, *refs):
    own, cosine, sine = refs[:3]
    more, out = refs[3 : 3 + n_more], refs[3 + n_more]
    length = own.shape[0]
    half = HEAD_SIZE // 2
    cos, sin = cosine[...], sine[...]

    def piece(start, width):
        total = own[:, start : start + width]
        for ref in more:
            total = total + ref[:, start : start + width].astype(F32)
        return total

    def rotate(u):
        first, second = u[:, :half], u[:, half:]
        return jnp.concatenate([first * cos - second * sin, second * cos + first * sin], axis=-1)

    q_width = heads * HEAD_SIZE
    key = rotate(piece(q_width, HEAD_SIZE).astype(BF16).astype(F32)).astype(BF16)
    value = piece(q_width + HEAD_SIZE, HEAD_SIZE).astype(BF16)
    rows = lax.broadcasted_iota(jnp.int32, (length, length), 0)
    columns = lax.broadcasted_iota(jnp.int32, (length, length), 1)
    causal = rows >= columns
    for head in range(heads):
        query = rotate(piece(head * HEAD_SIZE, HEAD_SIZE)).astype(BF16)
        score = lax.dot_general(
            query, key, (((1,), (1,)), ((), ())), preferred_element_type=F32
        ) * HEAD_SIZE ** (-0.5)
        score = 50.0 * jnp.tanh(score / 50.0)
        weight = jnp.where(causal, jnp.exp(score), 0.0)
        probs = (weight / jnp.sum(weight, axis=-1, keepdims=True)).astype(BF16)
        context = jnp.dot(probs, value, preferred_element_type=F32)
        out[:, head * HEAD_SIZE : (head + 1) * HEAD_SIZE] = context.astype(BF16)


def attend_call(own, more, cosine, sine, heads):
    length = own.shape[0]
    return pl.pallas_call(
        functools.partial(attend_body, len(more), heads),
        in_specs=[VM] * (3 + len(more)),
        out_specs=VM,
        out_shape=shape((length, heads * HEAD_SIZE), BF16),
        compiler_params=params(16),
        cost_estimate=cost(1e9, 4 * own.size),
        name="attend",
    )(own, cosine, sine, *more)


def project_body(cands, group, ids, cand_of, lambdas, *refs):
    contexts, base_far, task_far = refs[:cands], refs[cands], refs[cands + 1]
    keep, send, stack, base, task, sem = refs[cands + 2 :]
    loads = [
        pltpu.make_async_copy(base_far, base, sem.at[0]),
        pltpu.make_async_copy(task_far, task, sem.at[1]),
    ]
    for load in loads:
        load.start()
    own, bit = ids[0], ids[1]
    half = group // 2
    length, width = keep.shape[1:]
    for k in range(cands):
        stack[k * length : (k + 1) * length, :] = contexts[k][...]
    for load in loads:
        load.wait()
    for start in range(0, width, 256):
        cols = slice(start, min(start + 256, width))
        of_base = jnp.dot(stack[...], base[:, cols], preferred_element_type=F32)
        of_task = jnp.dot(stack[...], task[:, cols], preferred_element_type=F32)
        for k in range(cands):
            seq = own ^ k
            part, inside = seq // group, seq % group
            at = part * half + inside % half
            mixing = lambdas[cand_of[seq]]
            rows = slice(k * length, (k + 1) * length)
            result = of_base[rows] + mixing * of_task[rows]
            mine = inside // half == bit

            @pl.when(mine)
            def _():
                keep[at, :, cols] = result

            @pl.when(jnp.logical_not(mine))
            def _():
                send[at, :, cols] = result.astype(BF16)


def project_call(ids, cand_of, lambdas, contexts, base, task, group):
    cands = len(contexts)
    length, depth = contexts[0].shape
    width = base.shape[1]
    return pl.pallas_call(
        functools.partial(project_body, cands, group),
        in_specs=[SM] * 3 + [VM] * cands + [FAR] * 2,
        out_specs=[VM, VM],
        out_shape=[shape((cands // 2, length, width), F32), shape((cands // 2, length, width), BF16)],
        scratch_shapes=[
            pltpu.VMEM((cands * length, depth), BF16),
            pltpu.VMEM(base.shape, BF16),
            pltpu.VMEM(task.shape, BF16),
            pltpu.SemaphoreType.DMA((2,)),
        ],
        compiler_params=params(24),
        cost_estimate=cost(4 * cands * length * width * depth, 4 * base.size),
        name="project",
    )(ids, cand_of, lambdas, *contexts, base, task)


def spread_body(blocks, rows, ids, keep, got, own, *sends):
    at = ids[2]
    for mask in range(blocks):
        start = pl.multiple_of((at ^ mask) * rows, rows)
        total = keep[pl.ds(start, rows), :] + got[pl.ds(start, rows), :].astype(F32)
        if mask == 0:
            own[...] = total
        else:
            sends[mask - 1][...] = total.astype(BF16)


def spread_call(ids, keep, got, blocks):
    rows, width = keep.shape[0] // blocks, keep.shape[1]
    return pl.pallas_call(
        functools.partial(spread_body, blocks, rows),
        in_specs=[SM, VM, VM],
        out_specs=[VM] * blocks,
        out_shape=[shape((rows, width), F32)] + [shape((rows, width), BF16)] * (blocks - 1),
        compiler_params=params(8),
        cost_estimate=cost(1e9, 8 * keep.size),
        name="spread",
    )(ids, keep, got)


def sums_body(n_got, n_raw, rows, ids, own, gain, *refs):
    got, raw = refs[:n_got], refs[n_got : n_got + n_raw]
    attended, stream, sums = refs[n_got + n_raw :]
    a = own[...]
    for ref in got:
        a = a + ref[...].astype(F32)
    attended[...] = a
    take = min(rows, raw[0].shape[0] - TAIL)
    for step in range(rows // take):
        for k in range(n_raw):

            @pl.when(ids[step] == k)
            def _():
                start = pl.multiple_of(ids[rows // take], take)
                stream[step * take : (step + 1) * take, :] = raw[k][pl.ds(start, take), :]

    s = stream[...].astype(F32)
    ag = a * gain[...][:1]
    lanes = lax.broadcasted_iota(jnp.int32, sums.shape, 1)
    total = jnp.zeros(sums.shape, F32)
    for lane, term in enumerate((a * a, s * s, s * ag, ag * ag)):
        total = jnp.where(lanes == lane, jnp.sum(term, axis=1, keepdims=True), total)
    sums[...] = total


def sums_call(ids, own, got, raw, gain):
    rows, width = own.shape
    return pl.pallas_call(
        functools.partial(sums_body, len(got), len(raw), rows),
        in_specs=[SM] + [VM] * (2 + len(got) + len(raw)),
        out_specs=[VM] * 3,
        out_shape=[shape((rows, width), F32), shape((rows, width), BF16), shape((rows, 128), F32)],
        compiler_params=params(8),
        cost_estimate=cost(1e9, 8 * own.size),
        name="sums",
    )(ids, own, gain, *got, *raw)


def finish_body(features, n_sums, attended, stream, post, final, *refs):
    sums, out = refs[:n_sums], refs[n_sums]
    total = sums[0][...]
    for ref in sums[1:]:
        total = total + ref[...]
    aa, ss, sag, agag = (total[:, i : i + 1] / features for i in range(4))
    first = lax.rsqrt(aa + EPS)
    second = lax.rsqrt(ss + 2.0 * first * sag + first * first * agag + EPS)
    mixed = stream[...].astype(F32) + attended[...] * first * post[...][:1]
    out[...] = (mixed * second * final[...][:1]).astype(BF16)


def finish_call(attended, stream, post, final, sums, features):
    return pl.pallas_call(
        functools.partial(finish_body, features, len(sums)),
        in_specs=[VM] * (4 + len(sums)),
        out_specs=VM,
        out_shape=shape(attended.shape, BF16),
        compiler_params=params(8),
        cost_estimate=cost(1e9, 8 * attended.size),
        name="finish",
    )(attended, stream, post, final, *sums)


def vocab_body(n_pieces, blocks, rows, width, at, targets, *refs):
    pieces = refs[:n_pieces]
    unembed, out, x, sem, acc = refs[n_pieces : n_pieces + 5]
    step = pl.program_id(0)

    def copies():
        for p in range(n_pieces):
            for m in range(blocks):
                row = pl.multiple_of(at[p * (blocks + 1) + 1 + m] * rows, rows)
                col = pl.multiple_of(at[p * (blocks + 1)] * width, 128)
                yield pltpu.make_async_copy(
                    pieces[p].at[pl.ds(m * rows, rows), :],
                    x.at[pl.ds(row, rows), pl.ds(col, width)],
                    sem.at[p * blocks + m],
                )

    @pl.when(step == 0)
    def _():
        for copy in copies():
            copy.start()
        acc[...] = jnp.zeros_like(acc)
        for copy in copies():
            copy.wait()

    vocab_tile(step, targets, x, unembed, out, acc)


def vocab_tile(step, targets, x, unembed, out, acc):
    rows, tile = x.shape[0], unembed.shape[1]
    sub = tile_of(tile, 256, 128)
    local = targets[...] - step * tile
    columns = lax.broadcasted_iota(jnp.int32, (rows, 128), 1)
    totals = jnp.zeros((rows, 128), F32)
    picked = jnp.zeros((rows, 128), F32)
    for start in range(0, tile, sub):
        logits = jnp.dot(
            x[...], unembed[:, start : start + sub], preferred_element_type=F32
        )
        for lane in range(0, sub, 128):
            capped = 30.0 * jnp.tanh(logits[:, lane : lane + 128] / 30.0)
            totals += jnp.exp(capped)
            picked += jnp.where(columns == local - (start + lane), capped, 0.0)
    acc[:, :128] += totals
    acc[:, 128:] += picked

    @pl.when(step == pl.num_programs(0) - 1)
    def _():
        for row in range(2):
            turned = jnp.transpose(acc[:, row * 128 : (row + 1) * 128])
            out[row : row + 1, :] = jnp.sum(turned, axis=0, keepdims=True)


def vocab_plain_body(targets, x, unembed, out, acc):
    step = pl.program_id(0)

    @pl.when(step == 0)
    def _():
        acc[...] = jnp.zeros_like(acc)

    vocab_tile(step, targets, x, unembed, out, acc)


def vocab_call(pieces, places, targets, unembed, blocks):
    rows, width = pieces[0].shape[0] // blocks, pieces[0].shape[1]
    total_rows = targets.shape[0]
    features, vocab = unembed.shape
    tile = tile_of(vocab, 1024, 512, 256, 128)
    spec = dict(
        out_shape=shape((8, total_rows), F32),
        compiler_params=params(40),
        cost_estimate=cost(2 * total_rows * features * vocab, 2 * unembed.size),
        name="vocab",
    )
    if width % 128 == 0:
        full = pl.BlockSpec((8, total_rows), lambda i, *_: (0, 0))
        return pl.pallas_call(
            functools.partial(vocab_body, len(pieces), blocks, rows, width),
            grid_spec=pltpu.PrefetchScalarGridSpec(
                num_scalar_prefetch=1,
                grid=(vocab // tile,),
                in_specs=[pl.BlockSpec((total_rows, 1), lambda i, *_: (0, 0))]
                + [pl.BlockSpec(memory_space=pl.ANY)] * len(pieces)
                + [pl.BlockSpec((features, tile), lambda i, *_: (0, i))],
                out_specs=full,
                scratch_shapes=[
                    pltpu.VMEM((total_rows, features), BF16),
                    pltpu.SemaphoreType.DMA((len(pieces) * blocks,)),
                    pltpu.VMEM((total_rows, 256), F32),
                ],
            ),
            **spec,
        )(jnp.concatenate(places).astype(jnp.int32), targets, *pieces, unembed)
    x = jnp.zeros((total_rows, features), BF16)
    for piece, place in zip(pieces, places):
        for m in range(blocks):
            x = lax.dynamic_update_slice(
                x, piece[m * rows : (m + 1) * rows], (place[1 + m] * rows, place[0] * width)
            )
    return pl.pallas_call(
        vocab_plain_body,
        grid=(vocab // tile,),
        in_specs=[
            pl.BlockSpec((total_rows, 1), lambda i: (0, 0)),
            pl.BlockSpec((total_rows, features), lambda i: (0, 0)),
            pl.BlockSpec((features, tile), lambda i: (0, i)),
        ],
        out_specs=pl.BlockSpec((8, total_rows), lambda i: (0, 0)),
        scratch_shapes=[pltpu.VMEM((total_rows, 256), F32)],
        **spec,
    )(targets, x, unembed)


def on_device(
    states,
    targets,
    loss_mask,
    cand_of,
    lambdas,
    base_q,
    delta_q,
    base_k,
    delta_k,
    base_v,
    delta_v,
    base_o,
    delta_o,
    pre_gain,
    post_gain,
    final_gain,
    unembed,
):
    cands, tensors = lax.axis_size("cand"), lax.axis_size("tensor")
    own, place = lax.axis_index("cand"), lax.axis_index("tensor")
    length, features = states.shape
    width = features // cands
    tokens = cands * length
    heads = base_q.shape[1] // HEAD_SIZE
    blocks = tensors // 2
    bit, block = place % 2, place // 2
    head = place // (tensors // KV)

    ids = jnp.stack([own, head]).astype(jnp.int32)
    aligned = width % 128 == 0 and length == 128
    cuts = cut_call(ids, states, cands) if aligned else cut_plain(own, states, cands)
    xs = [cuts[0]] + [None] * (cands - 1)
    for k in [*range(2, cands), 1]:
        xs[k] = swap(cuts[k], "cand", k)

    weights, task_o = prep_call(
        ids, delta_q, [(base_k, delta_k), (base_v, delta_v)], delta_o
    )

    gains = jnp.stack([pre_gain, post_gain, final_gain])
    gains = lax.dynamic_slice_in_dim(gains, own * width, width, 1)
    gain, post, final = (jnp.broadcast_to(gains[i : i + 1], (8, width)) for i in range(3))
    partials = []
    after = []
    for first in range(0, cands, 2):
        inputs = xs[first : first + 2]
        if first:
            after = partials[-1:]
        partials += qkv_call(ids, cand_of, lambdas, inputs, gain, base_q, weights, first, after)
    crossed = [swap(partials[k + 1], "cand", 1) for k in range(0, cands, 2)]
    more = []
    for k in range(2, cands, 2):
        more.append(swap(join_call(partials[k], crossed[k // 2], BF16), "cand", k))

    positions = jnp.arange(length).astype(F32)
    half = HEAD_SIZE // 2
    frequency = jnp.exp(-math.log(10000.0) * jnp.arange(half).astype(F32) * 2.0 / HEAD_SIZE)
    angles = positions[:, None] * frequency[None, :]
    near = join_call(partials[0], crossed[0], F32)
    context = attend_call(near, more, jnp.cos(angles), jnp.sin(angles), heads)

    contexts = [None] * cands
    contexts[0] = context
    for k in range(2, cands, 2):
        contexts[k] = swap(context, "cand", k)
    for k in range(0, cands, 2):
        contexts[k + 1] = swap(contexts[k], "cand", 1)

    group = cands // PARTS
    keep, send = project_call(
        jnp.stack([own, bit]).astype(jnp.int32), cand_of, lambdas, contexts, base_o, task_o, group
    )
    part_rows = tokens // PARTS
    rows = part_rows // tensors
    spot = jnp.stack([own, bit, block]).astype(jnp.int32)
    arrived, results = [], []
    for part in range(PARTS):
        lo, hi = part * group // 2, (part + 1) * group // 2
        got = swap(send[lo:hi], "tensor", 1).reshape(part_rows // 2, width)
        mine, *sends = spread_call(spot, keep[lo:hi].reshape(part_rows // 2, width), got, blocks)
        got = [swap(sends[m - 1], "tensor", 2 * m) for m in range(1, blocks)]
        first_row = part * part_rows + (bit * blocks + block) * rows
        where = jnp.stack(
            [(first_row // length + i) ^ own for i in range(max(1, rows // length))]
            + [first_row % length]
        ).astype(jnp.int32)
        attended, s, sums = sums_call(where, mine, got, xs, post)
        every = [sums] + [swap(sums, "cand", k) for k in range(1, cands)]
        final_rows = finish_call(attended, s, post, final, every, features)
        pile = [final_rows] + [swap(final_rows, "tensor", 2 * m) for m in range(1, blocks)]
        pile = jnp.concatenate(pile, axis=0)
        crossing = []
        for cand_mask in range(0, cands, 2):
            for bit_mask in range(2):
                if cand_mask or bit_mask:
                    crossing.append(swap_both(pile, cand_mask, bit_mask))
                else:
                    crossing.append(pile)
        arrived.append(crossing)
    for part in range(PARTS):
        crossing = arrived[part]
        pieces, places = [], []
        for index, piece in enumerate(crossing):
            cand_mask, bit_mask = index // 2 * 2, index % 2
            for core_mask in range(2):
                if core_mask:
                    piece = swap(piece, "cand", 1)
                pieces.append(piece)
                places.append(
                    jnp.stack(
                        [own ^ cand_mask ^ core_mask]
                        + [(bit ^ bit_mask) * blocks + (block ^ m) for m in range(blocks)]
                    )
                )
        vocab_start = (own * tensors + place) * unembed.shape[1]
        ids_here = targets[part * part_rows : (part + 1) * part_rows] - vocab_start
        results.append(vocab_call(pieces, places, ids_here.reshape(part_rows, 1), unembed, blocks))
    both = jnp.concatenate(results, axis=1)[:2]
    masks = jnp.where(
        (lax.broadcasted_iota(jnp.int32, (cands, 1), 0) == own) & (place == 0),
        loss_mask.astype(F32)[None, :],
        0.0,
    ).reshape(1, tokens)
    payload = jnp.concatenate([both, masks], axis=0)
    payload = jnp.broadcast_to(payload[None], (cands * tensors,) + payload.shape)
    summed = jnp.sum(lax.all_to_all(payload, ("cand", "tensor"), 0, 0), axis=0)
    mask_values = summed[2]
    losses = mask_values * (jnp.log(summed[0]) - summed[1])
    token_loss = lax.dynamic_slice_in_dim(losses, own * length, length, 0)
    onehot = (cand_of[:, None] == jnp.arange(CANDS)[None, :]).astype(F32)
    loss_sums = jnp.sum(onehot * jnp.sum(losses.reshape(cands, length), axis=1)[:, None], axis=0)
    counts = jnp.sum(onehot * jnp.sum(mask_values.reshape(cands, length), axis=1)[:, None], axis=0)
    return (token_loss, loss_sums / jnp.maximum(counts, 1.0))


def solution(mesh):
    in_specs = (
        P("cand", None),
        P(),
        P("cand"),
        P(),
        P(),
        P("cand", "tensor"),
        P(None, "cand", "tensor"),
        P("cand", None),
        P(None, "cand", None),
        P("cand", None),
        P(None, "cand", None),
        P("tensor", "cand"),
        P(None, "tensor", "cand"),
        P(),
        P(),
        P(),
        P(None, ("cand", "tensor")),
    )
    out_specs = (P("cand"), P())

    return jax.shard_map(on_device, mesh=mesh, in_specs=in_specs, out_specs=out_specs, check_vma=False)
```
